32 devices in a mesh: sub: 16 (over z, x, core), chan: 2 (over y).
Axes of the slice: x: 2, y: 2, z: 4, core: 2. Of those that a mesh axis runs over, the one named last changes fastest.
Arguments:
- raw_pulses: bfloat16 [2, 512, 2, 2048], P(None, 'sub', 'chan'), may hold values from -6 to 6
- range_filter: bfloat16 [2, 2048, 1024], P(None, ('sub', 'chan')), may hold values from -0.09375 to 0.09375
- channel_mix: float32 [2, 32, 2, 2], replicated, may hold values from -3 to 3
- steer_angles: float32 [256], replicated, may hold values from -3.140625 to 3.140625
- band_offsets: int32 [4, 512], replicated, may hold values from 0 to 248
- band_weights: float32 [4, 2, 2, 512, 8], replicated, may hold values from -1 to 1
- smoothing: float32 [4096], P('sub'), may hold values from 0.3 to 0.5
Outputs:
- despeckled: float32 [4096, 1024], P('sub', 'chan')
The draws below stay inside these ranges and needn't reach their ends.
All inputs are finite; a program needn't handle non-finite values.
Results may differ from the reference program's by a relative error of at most 0.0036.
Values may be sent and summed in bfloat16 or wider, within the bound.
A program may use at most 64 MiB of HBM per device.

```python
import jax
import jax.numpy as jnp
import numpy as np
from jax import lax

P_DEV = 32
SAMPLES = 2048
BINS = 1024
ANG = 256
BAND = 8
LEVELS = 4
PASSES = 3
CHANNELS = 2
PULSES = 512
ANGLES = 4096
N_SUB = 16


def set_ends(entries, key, least, top_value):
    index_at = [jax.random.randint(jax.random.fold_in(key, axis), (), 0, length) for axis, length in enumerate(entries.shape)]
    main_axis = entries.shape.index(max(entries.shape))
    next_to = index_at[:main_axis] + [(index_at[main_axis] + 1) % entries.shape[main_axis]] + index_at[main_axis + 1:]
    return entries.at[tuple(index_at)].set(least).at[tuple(next_to)].set(top_value)


def level_of(own_key, extent, split, least, top_value):
    factor_of = 1.0
    for dim, parts in split:
        steps = jax.random.uniform(jax.random.fold_in(jax.random.fold_in(own_key, 6), dim), (parts,), jnp.float32, least / len(split), top_value / len(split))
        factor_of = factor_of * jnp.repeat(jnp.exp(steps), extent[dim] // parts).reshape((-1,) + (1,) * (len(extent) - 1 - dim))
    return factor_of


def scatter_about(own_key, extent, deviation, most, split=(), kind=jnp.bfloat16):
    loudness = level_of(own_key, extent, split, -0.22, 0.18) if split else 1.0
    values = jax.random.normal(own_key, extent, jnp.float32) * deviation * loudness
    return jnp.minimum(jnp.maximum(values, -most), most).astype(kind)


def setup_inputs(seed: int = 0) -> dict:
    keys = jax.random.split(jax.random.key(seed), 8)
    return {
        "raw_pulses": scatter_about(keys[0], (2, PULSES, CHANNELS, SAMPLES), 1.0, 6.0, ((1, 16), (2, 2))),
        "range_filter": scatter_about(keys[1], (2, SAMPLES, BINS), (2 * SAMPLES) ** -0.5, 0.09375, ((1, 32),)),
        "channel_mix": scatter_about(keys[2], (2, P_DEV, CHANNELS, CHANNELS), (2 * CHANNELS) ** -0.5, 3.0, (), jnp.float32),
        "steer_angles": jnp.clip(jax.random.uniform(keys[3], (ANG,), jnp.float32, -3.140625, 3.140625), -3.140625, 3.140625),
        "band_offsets": set_ends(jax.random.randint(keys[4], (LEVELS, 2 * ANG), 0, ANG - BAND + 1), jax.random.fold_in(keys[4], 1), 0, ANG - BAND).astype(jnp.int32),
        "band_weights": scatter_about(keys[5], (LEVELS, 2, 2, 2 * ANG, BAND), (4 * BAND) ** -0.5, 1.0, (), jnp.float32),
        "smoothing": jnp.clip(0.3 + 0.19999999 * jax.random.uniform(keys[6], (ANGLES,), jnp.float32) ** level_of(keys[6], (ANGLES,), ((0, 16),), -0.2, 0.2), 0.3, 0.5),
    }


HIGH = lax.Precision.HIGHEST

def doppler_table(count):
    index_row = jnp.arange(count, dtype=jnp.int32)
    product = index_row[:, None] * index_row[None, :] % count
    phase = 2.0 * np.pi / count * product.astype(jnp.float32)
    factor = 1.0 / np.sqrt(count)
    return ((jnp.cos(phase) * factor).astype(jnp.bfloat16), (-jnp.sin(phase) * factor).astype(jnp.bfloat16))

def steer_table(steer_angles, count):
    offsets = jnp.arange(count, dtype=jnp.int32).astype(jnp.float32) - 0.5 * count
    phase = steer_angles[:, None] * offsets[None, :]
    factor = 1.0 / np.sqrt(count)
    return ((jnp.cos(phase) * factor).astype(jnp.bfloat16), (jnp.sin(phase) * factor).astype(jnp.bfloat16))

def low_dot(left, right):
    return jnp.dot(left, right, preferred_element_type=jnp.float32)

def range_terms(echo_rows, filter_rows):
    real_part = low_dot(echo_rows[0], filter_rows[0]) - low_dot(echo_rows[1], filter_rows[1])
    imag_part = low_dot(echo_rows[0], filter_rows[1]) + low_dot(echo_rows[1], filter_rows[0])
    return jnp.stack([real_part, imag_part])

def form_image(compressed, dop_real, dop_imag, channel_mix, beam_real, beam_imag):
    pulse_count = compressed.shape[1]
    channels = compressed.shape[2]
    cells = compressed.shape[3]
    flat = compressed.reshape(2, pulse_count, channels * cells)
    spec_real = (low_dot(dop_real, flat[0]) - low_dot(dop_imag, flat[1])).reshape(pulse_count, channels, cells)
    spec_imag = (low_dot(dop_real, flat[1]) + low_dot(dop_imag, flat[0])).reshape(pulse_count, channels, cells)
    mix_real = jnp.einsum('fkc,fcb->kfb', channel_mix[0], spec_real, precision=HIGH) - jnp.einsum('fkc,fcb->kfb', channel_mix[1], spec_imag, precision=HIGH)
    mix_imag = jnp.einsum('fkc,fcb->kfb', channel_mix[0], spec_imag, precision=HIGH) + jnp.einsum('fkc,fcb->kfb', channel_mix[1], spec_real, precision=HIGH)
    recon = jnp.stack([mix_real, mix_imag]).astype(jnp.bfloat16).reshape(2, channels * pulse_count, cells)
    image_real = low_dot(beam_real, recon[0]) - low_dot(beam_imag, recon[1])
    image_imag = low_dot(beam_real, recon[1]) + low_dot(beam_imag, recon[0])
    return jnp.stack([image_real, image_imag])

def band_matrix(offsets, weights, count):
    band_width = weights.shape[-1]
    columns = jnp.arange(count, dtype=jnp.int32)
    stepping = jnp.arange(band_width, dtype=jnp.int32)
    target = offsets.astype(jnp.int32)[:, None, None] + stepping[None, :, None]
    hitting = (columns[None, None, :] == target).astype(jnp.float32)
    return jnp.einsum('crkj,kja->crka', weights, hitting, precision=HIGH)

def batched_apply(matrices, field):
    real_part = jnp.einsum('dka,dab->dkb', matrices[0], field[:, 0], precision=HIGH) - jnp.einsum('dka,dab->dkb', matrices[1], field[:, 1], precision=HIGH)
    imag_part = jnp.einsum('dka,dab->dkb', matrices[0], field[:, 1], precision=HIGH) + jnp.einsum('dka,dab->dkb', matrices[1], field[:, 0], precision=HIGH)
    return jnp.stack([real_part, imag_part], axis=1)

def reference(raw_pulses, range_filter, channel_mix, steer_angles, band_offsets, band_weights, smoothing):
    channels = raw_pulses.shape[2]
    blocks = jnp.moveaxis(raw_pulses.reshape(2, N_SUB, P_DEV, channels, SAMPLES), 1, 0)
    dop_real, dop_imag = doppler_table(P_DEV)
    beam_real, beam_imag = steer_table(steer_angles, channels * P_DEV)

    def one_block(block):
        echo_rows = block.reshape(2, P_DEV * channels, SAMPLES)
        compressed = range_terms(echo_rows, range_filter).astype(jnp.bfloat16).reshape(2, P_DEV, channels, BINS)
        return form_image(compressed, dop_real, dop_imag, channel_mix, beam_real, beam_imag)
    images = lax.map(one_block, blocks)
    index_all = np.arange(N_SUB)
    for merge_level in range(LEVELS):
        bit_value = 1 << merge_level
        lower_index = index_all & ~bit_value
        upper_index = index_all | bit_value
        half_index = index_all >> merge_level & 1
        full_band = band_matrix(band_offsets[merge_level], band_weights[merge_level], ANG)
        full_band = full_band.reshape(2, 2, 2, ANG, ANG)
        chosen = full_band[:, :, half_index]
        images = batched_apply(chosen[0], images[lower_index]) + batched_apply(chosen[1], images[upper_index])
    power = images[:, 0] * images[:, 0] + images[:, 1] * images[:, 1]
    power = power.reshape(N_SUB * ANG, BINS)
    rate = smoothing[:, None]
    for sweep in range(PASSES):
        padded = jnp.pad(power, ((0, 0), (1, 1)))
        power = power + rate * (padded[:, :-2] - 2.0 * power + padded[:, 2:])
    return power
```

```python
import jax
import jax.numpy as jnp
import numpy as np
from jax import lax
from jax.sharding import PartitionSpec as P

PASSES = 3
HIGH = lax.Precision.HIGHEST
LOW = jnp.bfloat16


def rounded(value):
    return lax.reduce_precision(value, exponent_bits=8, mantissa_bits=7)


def halves(value):
    top = rounded(value)
    return top.astype(LOW), (value - top).astype(LOW)


def doppler_table(count):
    index_row = jnp.arange(count, dtype=jnp.int32)
    product = index_row[:, None] * index_row[None, :] % count
    phase = 2.0 * np.pi / count * product.astype(jnp.float32)
    factor = 1.0 / np.sqrt(count)
    return (
        rounded(jnp.cos(phase) * factor),
        rounded(-jnp.sin(phase) * factor),
    )


def steer_table(steer_angles, count):
    offsets = jnp.arange(count, dtype=jnp.int32).astype(jnp.float32) - 0.5 * count
    phase = offsets[:, None] * steer_angles[None, :]
    factor = 1.0 / np.sqrt(count)
    return (
        rounded(jnp.cos(phase) * factor),
        rounded(jnp.sin(phase) * factor),
    )


def forming_operator(channel_mix, steer_angles, pulse_count):
    channels = channel_mix.shape[2]
    dop_r, dop_i = doppler_table(pulse_count)
    beam_r, beam_i = steer_table(steer_angles, channels * pulse_count)
    mix = channel_mix.transpose(0, 3, 2, 1)[:, :, None, :, :]
    dr, di = dop_r.T[None, :, None, :], dop_i.T[None, :, None, :]
    shape = (channels * pulse_count, channels * pulse_count)
    mixed_r = (mix[0] * dr - mix[1] * di).reshape(shape)
    mixed_i = (mix[0] * di + mix[1] * dr).reshape(shape)
    left = jnp.concatenate([mixed_r, mixed_i], axis=1)
    t_r = jnp.dot(left, jnp.concatenate([beam_r, -beam_i], axis=0), precision=HIGH)
    t_i = jnp.dot(left, jnp.concatenate([beam_i, beam_r], axis=0), precision=HIGH)
    angles = steer_angles.shape[0]
    t_r = t_r.reshape(channels, pulse_count, angles)
    t_i = t_i.reshape(channels, pulse_count, angles)
    top = jnp.concatenate([t_r, t_i], axis=2)
    low = jnp.concatenate([-t_i, t_r], axis=2)
    both = jnp.concatenate([top, low], axis=1)
    return both.reshape(channels * 2 * pulse_count, 2 * angles)


def merge_operator(offsets, weights, count):
    band_width = weights.shape[-1]
    rows = jnp.arange(count, dtype=jnp.int32)
    delta = rows[:, None] - offsets[None, :]
    band = jnp.zeros(weights.shape[:2] + delta.shape, jnp.float32)
    for j in range(band_width):
        band = jnp.where(delta == j, weights[:, :, None, :, j], band)
    band = band.reshape(weights.shape[:2] + (count, -1, 1, count))
    top = jnp.concatenate([band[:, 0], band[:, 1]], axis=3)
    low = jnp.concatenate([-band[:, 1], band[:, 0]], axis=3)
    both = jnp.concatenate([top, low], axis=1)
    return both.reshape(both.shape[0], 2 * count, -1)


def low_dot(left, right):
    return jnp.dot(left, right, preferred_element_type=jnp.float32)


def local(
    raw_pulses, range_filter, channel_mix, steer_angles, band_offsets, band_weights, smoothing
):
    pulses = raw_pulses.shape[1]
    samples = raw_pulses.shape[3]
    bins = range_filter.shape[2]
    angles = steer_angles.shape[0]
    levels = band_offsets.shape[0]
    subs, chans = lax.axis_size("sub"), lax.axis_size("chan")
    own = bins // (subs * chans)

    filt = lax.all_gather(range_filter, ("sub", "chan"), axis=1, tiled=True)
    forming = forming_operator(channel_mix, steer_angles, pulses)
    merging = []
    for level in range(levels):
        weights = merge_operator(band_offsets[level], band_weights[level], angles)
        if level == 0:
            weights = jnp.einsum("ij,cjk->cik", forming, weights, precision=HIGH)
        merging.append(halves(weights.reshape(-1, 4 * angles)))

    echo = raw_pulses[:, :, 0, :]
    real_rows = jnp.concatenate([echo[0], -echo[1]], axis=1)
    imag_rows = jnp.concatenate([echo[1], echo[0]], axis=1)
    stacked = jnp.concatenate([real_rows, imag_rows], axis=0)
    compressed = low_dot(stacked, filt.reshape(2 * samples, bins)).astype(LOW)
    blocks = compressed.T.reshape(chans, subs, own, 2 * pulses)
    blocks = blocks.reshape(chans * subs, own * 2 * pulses // 128, 128)
    got = lax.all_to_all(blocks, ("chan", "sub"), split_axis=0, concat_axis=0, tiled=True)
    got = got.reshape(chans, subs * own, 2 * pulses)

    image = jnp.concatenate([got[c] for c in range(chans)], axis=1)
    for level in range(levels):
        run = (1 << level) * own
        wide = image.shape[1]
        field = image.astype(LOW).reshape(-1, 2, run, wide)
        pair = jnp.concatenate([field[:, 0], field[:, 1]], axis=2).reshape(-1, 2 * wide)
        out = low_dot(pair, merging[level][0]) + low_dot(pair, merging[level][1])
        out = out.reshape(-1, run, 4 * angles)
        image = jnp.stack([out[:, :, : 2 * angles], out[:, :, 2 * angles :]], axis=1)
        image = image.reshape(-1, 2 * angles)
    power = image[:, :angles] * image[:, :angles] + image[:, angles:] * image[:, angles:]
    power = power.astype(LOW).reshape(subs, own, angles)
    power = lax.all_to_all(power, "sub", split_axis=0, concat_axis=0, tiled=True)
    power = power.reshape(subs * own, angles)
    up = [(i, i + 1) for i in range(chans - 1)]
    down = [(j, i) for i, j in up]
    before = lax.ppermute(power[-PASSES:], "chan", up).astype(jnp.float32)
    after = lax.ppermute(power[:PASSES], "chan", down).astype(jnp.float32)
    power = jnp.concatenate([before, power.astype(jnp.float32), after], axis=0)
    rate = smoothing[None, :]
    at = lax.axis_index("chan")
    lead, trail = at == 0, at == chans - 1
    for sweep in range(PASSES):
        mid = power[1:-1]
        power = mid + rate * (power[:-2] - 2.0 * mid + power[2:])
        edge = PASSES - 1 - sweep
        if edge:
            inner = power[edge:-edge]
            head = jnp.where(lead, 0.0, power[:edge])
            tail = jnp.where(trail, 0.0, power[-edge:])
            power = jnp.concatenate([head, inner, tail], axis=0)
    return power.T


def solution(mesh):
    in_specs = (
        P(None, "sub", "chan", None),
        P(None, ("sub", "chan"), None),
        P(),
        P(),
        P(),
        P(),
        P("sub"),
    )
    out_specs = P("sub", "chan")
    return jax.shard_map(local, mesh=mesh, in_specs=in_specs, out_specs=out_specs, check_vma=False)
```

```python
import jax
import jax.numpy as jnp
import numpy as np
from jax import lax
from jax.experimental import pallas as pl
from jax.sharding import PartitionSpec as P

PASSES = 3
HIGH = lax.Precision.HIGHEST
LOW = jnp.bfloat16


def rounded(value):
    return lax.reduce_precision(value, exponent_bits=8, mantissa_bits=7)


def halves(value):
    top = rounded(value)
    return top.astype(LOW), (value - top).astype(LOW)


def doppler_table(count):
    index_row = jnp.arange(count, dtype=jnp.int32)
    product = index_row[:, None] * index_row[None, :] % count
    phase = 2.0 * np.pi / count * product.astype(jnp.float32)
    factor = 1.0 / np.sqrt(count)
    return (
        rounded(jnp.cos(phase) * factor),
        rounded(-jnp.sin(phase) * factor),
    )


def steer_table(steer_angles, count):
    offsets = jnp.arange(count, dtype=jnp.int32).astype(jnp.float32) - 0.5 * count
    phase = offsets[:, None] * steer_angles[None, :]
    factor = 1.0 / np.sqrt(count)
    return (
        rounded(jnp.cos(phase) * factor),
        rounded(jnp.sin(phase) * factor),
    )


def forming_operator(channel_mix, steer_angles, pulse_count):
    channels = channel_mix.shape[2]
    dop_r, dop_i = doppler_table(pulse_count)
    beam_r, beam_i = steer_table(steer_angles, channels * pulse_count)
    mix = channel_mix.transpose(0, 3, 2, 1)[:, :, None, :, :]
    dr, di = dop_r.T[None, :, None, :], dop_i.T[None, :, None, :]
    shape = (channels * pulse_count, channels * pulse_count)
    mixed_r = (mix[0] * dr - mix[1] * di).reshape(shape)
    mixed_i = (mix[0] * di + mix[1] * dr).reshape(shape)
    left = jnp.concatenate([mixed_r, mixed_i], axis=1)
    t_r = jnp.dot(left, jnp.concatenate([beam_r, -beam_i], axis=0), precision=HIGH)
    t_i = jnp.dot(left, jnp.concatenate([beam_i, beam_r], axis=0), precision=HIGH)
    angles = steer_angles.shape[0]
    t_r = t_r.reshape(channels, pulse_count, angles)
    t_i = t_i.reshape(channels, pulse_count, angles)
    top = jnp.concatenate([t_r, t_i], axis=2)
    low = jnp.concatenate([-t_i, t_r], axis=2)
    both = jnp.concatenate([top, low], axis=1)
    return both.reshape(channels * 2 * pulse_count, 2 * angles)


def operator_body(offsets_ref, weights_ref, *out_refs):
    band_width, count = weights_ref.shape[3], weights_ref.shape[4]
    delta = lax.broadcasted_iota(jnp.int32, (count, count), 0) - offsets_ref[0]
    bands = [jnp.zeros((count, count), jnp.float32)] * 2
    for j in range(band_width):
        hit = delta == j
        bands = [
            jnp.where(hit, weights_ref[0, 0, part, j : j + 1, :], bands[part]) for part in range(2)
        ]
    for order, ref in enumerate(out_refs):
        real, imag = (band.astype(LOW) for band in bands)
        ref[0, 0, :count, :count] = real
        ref[0, 0, :count, count:] = imag
        ref[0, 0, count:, :count] = -imag
        ref[0, 0, count:, count:] = real
        if order + 1 < len(out_refs):
            bands = [band - band.astype(LOW).astype(jnp.float32) for band in bands]


def merge_operators(offsets, weights, parts):
    levels, _, _, merged, band_width = weights.shape
    count = merged // 2
    by_step = weights.transpose(0, 1, 2, 4, 3)
    shape = jax.ShapeDtypeStruct((levels, 2, 2 * count, 2 * merged), LOW)
    return pl.pallas_call(
        operator_body,
        grid=(levels, 2, 2),
        in_specs=[
            pl.BlockSpec((1, 1, count), lambda l, c, h: (l, 0, h)),
            pl.BlockSpec((1, 1, 2, band_width, count), lambda l, c, h: (l, c, 0, 0, h)),
        ],
        out_specs=[
            pl.BlockSpec((1, 1, 2 * count, 2 * count), lambda l, c, h: (l, c, 0, h))
        ] * parts,
        out_shape=[shape] * parts,
        cost_estimate=pl.CostEstimate(
            flops=levels * 4 * count * count * 32,
            bytes_accessed=levels * parts * 16 * count * count * 2,
            transcendentals=0,
        ),
    )(offsets[:, None, :], by_step)


def low_dot(left, right):
    return jnp.dot(left, right, preferred_element_type=jnp.float32)


def local(
    raw_pulses, range_filter, channel_mix, steer_angles, band_offsets, band_weights, smoothing
):
    pulses = raw_pulses.shape[1]
    samples = raw_pulses.shape[3]
    bins = range_filter.shape[2]
    angles = steer_angles.shape[0]
    levels = band_offsets.shape[0]
    subs, chans = lax.axis_size("sub"), lax.axis_size("chan")
    own = bins // (subs * chans)

    part = lax.all_to_all(range_filter, "chan", split_axis=2, concat_axis=1, tiled=True)
    filt = lax.all_gather(part, "sub", axis=1, tiled=True)
    echo = lax.all_gather(raw_pulses[:, :, 0, :], "chan", axis=0)

    forming = forming_operator(channel_mix, steer_angles, pulses)
    form_top, form_low = halves(forming)
    base_top, base_low = merge_operators(band_offsets[:1], band_weights[:1], 2)
    folded = [
        low_dot(form_top, base_top[0, c])
        + (low_dot(form_low, base_top[0, c]) + low_dot(form_top, base_low[0, c]))
        for c in range(2)
    ]
    folded_top, folded_low = halves(jnp.concatenate(folded, axis=0))
    (later,) = merge_operators(band_offsets[1:], band_weights[1:], 1)

    real_rows = jnp.concatenate([echo[:, 0], -echo[:, 1]], axis=2)
    imag_rows = jnp.concatenate([echo[:, 1], echo[:, 0]], axis=2)
    stacked = jnp.concatenate([real_rows, imag_rows], axis=1).reshape(-1, 2 * samples)
    compressed = low_dot(stacked, filt.reshape(2 * samples, -1)).astype(LOW)
    blocks = compressed.T.reshape(subs, own, -1)
    got = lax.all_to_all(blocks, "sub", split_axis=0, concat_axis=0, tiled=True)
    image = got.reshape(subs * own, -1)
    for level in range(levels):
        run = (1 << level) * own
        wide = image.shape[1]
        field = image.astype(LOW).reshape(-1, 2, run, wide)
        pair = jnp.concatenate([field[:, 0], field[:, 1]], axis=2).reshape(-1, 2 * wide)
        if level == 0:
            out = low_dot(pair, folded_top) + low_dot(pair, folded_low)
        else:
            out = low_dot(pair, later[level - 1].reshape(2 * wide, -1))
        out = out.reshape(-1, run, 4 * angles)
        image = jnp.stack([out[:, :, : 2 * angles], out[:, :, 2 * angles :]], axis=1)
        image = image.reshape(-1, 2 * angles)
    power = image[:, :angles] * image[:, :angles] + image[:, angles:] * image[:, angles:]
    power = power.astype(LOW).reshape(subs, own, angles)
    power = lax.all_to_all(power, "sub", split_axis=0, concat_axis=0, tiled=True)
    power = power.reshape(subs * own, angles)
    up = [(i, i + 1) for i in range(chans - 1)]
    down = [(j, i) for i, j in up]
    before = lax.ppermute(power[-PASSES:], "chan", up).astype(jnp.float32)
    after = lax.ppermute(power[:PASSES], "chan", down).astype(jnp.float32)
    power = jnp.concatenate([before, power.astype(jnp.float32), after], axis=0)
    rate = smoothing[None, :]
    at = lax.axis_index("chan")
    lead, trail = at == 0, at == chans - 1
    for sweep in range(PASSES):
        mid = power[1:-1]
        power = mid + rate * (power[:-2] - 2.0 * mid + power[2:])
        edge = PASSES - 1 - sweep
        if edge:
            inner = power[edge:-edge]
            head = jnp.where(lead, 0.0, power[:edge])
            tail = jnp.where(trail, 0.0, power[-edge:])
            power = jnp.concatenate([head, inner, tail], axis=0)
    return power.T


def solution(mesh):
    in_specs = (
        P(None, "sub", "chan", None),
        P(None, ("sub", "chan"), None),
        P(),
        P(),
        P(),
        P(),
        P("sub"),
    )
    out_specs = P("sub", "chan")
    return jax.shard_map(local, mesh=mesh, in_specs=in_specs, out_specs=out_specs, check_vma=False)
```

```python
import jax
import jax.numpy as jnp
import numpy as np
from jax import lax
from jax.experimental import pallas as pl
from jax.sharding import Mesh, PartitionSpec as P

PASSES = 3
HIGH = lax.Precision.HIGHEST
LOW = jnp.bfloat16


def rounded(value):
    return lax.reduce_precision(value, exponent_bits=8, mantissa_bits=7)


def halves(value):
    top = rounded(value)
    return top.astype(LOW), (value - top).astype(LOW)


def doppler_table(count):
    index_row = jnp.arange(count, dtype=jnp.int32)
    product = index_row[:, None] * index_row[None, :] % count
    phase = 2.0 * np.pi / count * product.astype(jnp.float32)
    factor = 1.0 / np.sqrt(count)
    return (
        rounded(jnp.cos(phase) * factor),
        rounded(-jnp.sin(phase) * factor),
    )


def steer_table(steer_angles, count):
    offsets = jnp.arange(count, dtype=jnp.int32).astype(jnp.float32) - 0.5 * count
    phase = offsets[:, None] * steer_angles[None, :]
    factor = 1.0 / np.sqrt(count)
    return (
        rounded(jnp.cos(phase) * factor),
        rounded(jnp.sin(phase) * factor),
    )


def forming_operator(channel_mix, steer_angles, pulse_count):
    channels = channel_mix.shape[2]
    dop_r, dop_i = doppler_table(pulse_count)
    beam_r, beam_i = steer_table(steer_angles, channels * pulse_count)
    mix = channel_mix.transpose(0, 3, 2, 1)[:, :, None, :, :]
    dr, di = dop_r.T[None, :, None, :], dop_i.T[None, :, None, :]
    shape = (channels * pulse_count, channels * pulse_count)
    mixed_r = (mix[0] * dr - mix[1] * di).reshape(shape)
    mixed_i = (mix[0] * di + mix[1] * dr).reshape(shape)
    left = jnp.concatenate([mixed_r, mixed_i], axis=1)
    t_r = jnp.dot(left, jnp.concatenate([beam_r, -beam_i], axis=0), precision=HIGH)
    t_i = jnp.dot(left, jnp.concatenate([beam_i, beam_r], axis=0), precision=HIGH)
    angles = steer_angles.shape[0]
    t_r = t_r.reshape(channels, pulse_count, angles)
    t_i = t_i.reshape(channels, pulse_count, angles)
    top = jnp.concatenate([t_r, t_i], axis=2)
    low = jnp.concatenate([-t_i, t_r], axis=2)
    both = jnp.concatenate([top, low], axis=1)
    return both.reshape(channels * 2 * pulse_count, 2 * angles)


def operator_body(offsets_ref, weights_ref, *out_refs):
    band_width, count = weights_ref.shape[3], weights_ref.shape[4]
    delta = lax.broadcasted_iota(jnp.int32, (count, count), 0) - offsets_ref[0]
    bands = [jnp.zeros((count, count), jnp.float32)] * 2
    for j in range(band_width):
        hit = delta == j
        bands = [
            jnp.where(hit, weights_ref[0, 0, part, j : j + 1, :], bands[part]) for part in range(2)
        ]
    for order, ref in enumerate(out_refs):
        real, imag = (band.astype(LOW) for band in bands)
        ref[0, 0, :count, :count] = real
        ref[0, 0, :count, count:] = imag
        ref[0, 0, count:, :count] = -imag
        ref[0, 0, count:, count:] = real
        if order + 1 < len(out_refs):
            bands = [band - band.astype(LOW).astype(jnp.float32) for band in bands]


def merge_operators(offsets, weights, parts):
    levels, _, _, merged, band_width = weights.shape
    count = merged // 2
    by_step = weights.transpose(0, 1, 2, 4, 3)
    shape = jax.ShapeDtypeStruct((levels, 2, 2 * count, 2 * merged), LOW)
    return pl.pallas_call(
        operator_body,
        grid=(levels, 2, 2),
        in_specs=[
            pl.BlockSpec((1, 1, count), lambda l, c, h: (l, 0, h)),
            pl.BlockSpec((1, 1, 2, band_width, count), lambda l, c, h: (l, c, 0, 0, h)),
        ],
        out_specs=[
            pl.BlockSpec((1, 1, 2 * count, 2 * count), lambda l, c, h: (l, c, 0, h))
        ] * parts,
        out_shape=[shape] * parts,
        cost_estimate=pl.CostEstimate(
            flops=levels * 4 * count * count * 32,
            bytes_accessed=levels * parts * 16 * count * count * 2,
            transcendentals=0,
        ),
    )(offsets[:, None, :], by_step)


def low_dot(left, right):
    return jnp.dot(left, right, preferred_element_type=jnp.float32)


def local(
    raw_pulses, range_filter, channel_mix, steer_angles, band_offsets, band_weights, smoothing
):
    pulses = raw_pulses.shape[1]
    samples = raw_pulses.shape[3]
    bins = range_filter.shape[2]
    angles = steer_angles.shape[0]
    levels = band_offsets.shape[0]
    pairs, cores, chans = (lax.axis_size(name) for name in ("pair", "core", "chan"))
    subs = pairs * cores
    own = bins // (subs * chans)

    near = ("core", "chan")
    split = range_filter.reshape(2, -1, chans, cores, pairs * own).swapaxes(2, 3)
    split = split.reshape(range_filter.shape)
    part = lax.all_to_all(split, near, split_axis=2, concat_axis=1, tiled=True)
    filt = lax.all_gather(part, "pair", axis=1, tiled=True)
    echo = lax.all_gather(raw_pulses[:, :, 0, :], near, axis=0)

    forming = forming_operator(channel_mix, steer_angles, pulses)
    form_top, form_low = halves(forming)
    base_top, base_low = merge_operators(band_offsets[:1], band_weights[:1], 2)
    folded = [
        low_dot(form_top, base_top[0, c])
        + (low_dot(form_low, base_top[0, c]) + low_dot(form_top, base_low[0, c]))
        for c in range(2)
    ]
    folded_top, folded_low = halves(jnp.concatenate(folded, axis=0))
    (later,) = merge_operators(band_offsets[1:], band_weights[1:], 1)

    real_rows = jnp.concatenate([echo[:, 0], -echo[:, 1]], axis=2)
    imag_rows = jnp.concatenate([echo[:, 1], echo[:, 0]], axis=2)
    stacked = jnp.concatenate([real_rows, imag_rows], axis=1).reshape(-1, 2 * samples)
    compressed = low_dot(stacked, filt.reshape(2 * samples, -1)).astype(LOW)
    blocks = compressed.T.reshape(pairs, own, -1)
    got = lax.all_to_all(blocks, "pair", split_axis=0, concat_axis=0, tiled=True)
    for level in range(levels):
        run = (1 << level) * own
        if level == 0:
            pair = got.reshape(pairs * own, -1)
            out = low_dot(pair, folded_top) + low_dot(pair, folded_low)
        else:
            wide = image.shape[1]
            field = image.astype(LOW).reshape(-1, 2, run, wide)
            pair = jnp.concatenate([field[:, 0], field[:, 1]], axis=2).reshape(-1, 2 * wide)
            out = low_dot(pair, later[level - 1].reshape(2 * wide, -1))
        out = out.reshape(-1, run, 4 * angles)
        image = jnp.stack([out[:, :, : 2 * angles], out[:, :, 2 * angles :]], axis=1)
        image = image.reshape(-1, 2 * angles)
    power = image[:, :angles] * image[:, :angles] + image[:, angles:] * image[:, angles:]
    power = power.astype(LOW).reshape(subs, own, angles)
    power = lax.all_to_all(power, ("pair", "core"), split_axis=0, concat_axis=0, tiled=True)
    power = power.reshape(pairs, cores, own, angles).swapaxes(0, 1).reshape(subs * own, angles)
    up = [(i, i + 1) for i in range(chans - 1)]
    down = [(j, i) for i, j in up]
    before = lax.ppermute(power[-PASSES:], "chan", up).astype(jnp.float32)
    after = lax.ppermute(power[:PASSES], "chan", down).astype(jnp.float32)
    power = jnp.concatenate([before, power.astype(jnp.float32), after], axis=0)
    rate = smoothing[None, :]
    at = lax.axis_index("chan")
    lead, trail = at == 0, at == chans - 1
    for sweep in range(PASSES):
        mid = power[1:-1]
        power = mid + rate * (power[:-2] - 2.0 * mid + power[2:])
        edge = PASSES - 1 - sweep
        if edge:
            inner = power[edge:-edge]
            head = jnp.where(lead, 0.0, power[:edge])
            tail = jnp.where(trail, 0.0, power[-edge:])
            power = jnp.concatenate([head, inner, tail], axis=0)
    return power.T


def solution(mesh):
    devices = mesh.devices
    grid = devices.reshape(devices.shape[0] // 2, 2, devices.shape[1])
    split_mesh = Mesh(grid, ("pair", "core", "chan"))
    sub = ("pair", "core")
    in_specs = (
        P(None, sub, "chan", None),
        P(None, ("pair", "core", "chan"), None),
        P(),
        P(),
        P(),
        P(),
        P(sub),
    )
    return jax.shard_map(
        local, mesh=split_mesh, in_specs=in_specs, out_specs=P(sub, "chan"), check_vma=False
    )
```
